64 devices in a mesh: rep: 8 (over x, y, core), dp: 8 (over z).
Axes of the slice: x: 2, y: 2, z: 8, core: 2. Of those that a mesh axis runs over, the one named last changes fastest.
The devices are a block of a 4x4x8 slice.
Arguments:
- x: bfloat16 [64, 2048, 768], P(('rep', 'dp')), parts along dimension 0
- dy: bfloat16 [64, 2048, 768], P(('rep', 'dp')), parts along dimension 0
- w_gate: bfloat16 [2, 768, 2048], replicated
- w_up: bfloat16 [2, 768, 2048], replicated
- w_down: bfloat16 [2, 2048, 768], replicated
- m_w_gate: float32 [2, 768, 2048], P(None, 'dp')
- m_w_up: float32 [2, 768, 2048], P(None, 'dp')
- m_w_down: float32 [2, 2048, 768], P(None, 'dp')
- v_w_gate: float32 [2, 768, 2048], P(None, 'dp')
- v_w_up: float32 [2, 768, 2048], P(None, 'dp')
- v_w_down: float32 [2, 2048, 768], P(None, 'dp')
Outputs:
- output 1: bfloat16 [16, 768, 2048], P('rep'), parts along dimension 0
- output 2: bfloat16 [16, 768, 2048], P('rep'), parts along dimension 0
- output 3: bfloat16 [16, 2048, 768], P('rep'), parts along dimension 0
- output 4: float32 [16, 768, 2048], P('rep', 'dp'), parts along dimension 0
- output 5: float32 [16, 768, 2048], P('rep', 'dp'), parts along dimension 0
- output 6: float32 [16, 2048, 768], P('rep', 'dp'), parts along dimension 0
- output 7: float32 [16, 768, 2048], P('rep', 'dp'), parts along dimension 0
- output 8: float32 [16, 768, 2048], P('rep', 'dp'), parts along dimension 0
- output 9: float32 [16, 2048, 768], P('rep', 'dp'), parts along dimension 0
There are 8 independent parts. The reference program is written for one: setup_inputs(seed, part) draws one part's arguments, and reference() takes and returns one part's arrays. A program takes and returns all parts, laid end to end along the dimension named above; an argument that names none is the same for every part.
All inputs are finite; a program needn't handle non-finite values.
Results may differ from the reference program's by a relative error of at most 0.022.
Values are sent between devices in bfloat16 or wider.
A program may use at most 768 MiB of HBM per device.

```python
import jax
import jax.numpy as jnp
from jax import lax

SEQUENCES = 8
TOKENS = 2048
D = 768
FF = 2048
LAYERS = 2
NAMES = ("w_gate", "w_up", "w_down")
SHAPES = {"w_gate": (LAYERS, D, FF), "w_up": (LAYERS, D, FF), "w_down": (LAYERS, FF, D)}


def bump(key, n, height):
    away = (jnp.arange(n, dtype=jnp.int32) - jax.random.randint(key, (), 0, n, jnp.int32)) % n
    return jnp.where(away < n // 8, height, 1.0)


def together(key, own, strength):
    shared = jax.random.normal(key, own.shape[1:], jnp.float32)
    return (own + strength * shared) * lax.rsqrt(1 + strength * strength)


def setup_inputs(seed: int = 0, part: int = 0) -> dict:
    kx, kdy, ka, kb, kz, kf, kh, kl, *keys = jax.random.split(jax.random.key(seed), 8 + 3 * len(NAMES))
    kx, kdy, ka, kb = (jax.random.fold_in(k, part) for k in (kx, kdy, ka, kb))
    kw, km, kv = (keys[i::3] for i in range(3))
    shape = (SEQUENCES, TOKENS, D)
    much_x, much_dy = jax.random.uniform(kz, (2,), jnp.float32, 0.0, 1.0)
    loud = 2.0 ** jax.random.uniform(jax.random.fold_in(kz, 1), (), jnp.float32, -1.0, 2.0)
    layers = 2.0 ** jax.random.uniform(kl, (LAYERS, 1, 1), jnp.float32, -1.0, 1.0)
    x = together(ka, jax.random.normal(kx, shape, jnp.float32), much_x) * bump(kf, D, 4.0)
    dy = together(kb, jax.random.normal(kdy, shape, jnp.float32), much_dy)
    drawn = {"x": x.astype(jnp.bfloat16), "dy": (loud * dy * (SEQUENCES * TOKENS) ** -0.5).astype(jnp.bfloat16)}
    for key, name in zip(kw, NAMES, strict=True):
        w = jax.random.normal(key, SHAPES[name], jnp.float32) * SHAPES[name][1] ** -0.5
        drawn[name] = (w * {"w_gate": 1.0, "w_up": bump(kh, FF, 4.0), "w_down": layers}[name]).astype(jnp.bfloat16)
    for key, name in zip(km, NAMES, strict=True):
        drawn[f"m_{name}"] = 0.1 * jax.random.normal(key, SHAPES[name], jnp.float32)
    for key, name in zip(kv, NAMES, strict=True):
        drawn[f"v_{name}"] = jax.random.uniform(key, SHAPES[name], jnp.float32, 0.005, 0.015)
    return drawn


def matmul(a, w):
    return jnp.dot(a, w, preferred_element_type=jnp.float32).astype(jnp.bfloat16)


def normed(h):
    wide = h.astype(jnp.float32)
    scale = lax.rsqrt(jnp.mean(wide**2, -1, keepdims=True) + 1e-6)
    return (wide * scale).astype(jnp.bfloat16)


def layer(h, w):
    a = normed(h)
    gate = jnp.dot(a, w["w_gate"], preferred_element_type=jnp.float32)
    up = jnp.dot(a, w["w_up"], preferred_element_type=jnp.float32)
    return h + matmul((jax.nn.silu(gate) * up).astype(jnp.bfloat16), w["w_down"])


def adamw(w, m, v, g):
    m = 0.9 * m + 0.1 * g
    v = 0.95 * v + 0.05 * g * g
    step = m * lax.rsqrt(v + 1e-8) + 0.1 * w
    return (w - 0.02 * step).astype(jnp.bfloat16), m, v


def clipped(gradients, sum_of_squares, count):
    factor = jnp.minimum(1.0, 0.5 * lax.rsqrt(sum_of_squares / count + 1e-30))
    return [g * factor for g in gradients]


def stack(weights, h):
    return lax.scan(lambda h, w: (layer(h, w), None), h, weights)[0]


def reference(x, dy, w_gate, w_up, w_down, m_w_gate, m_w_up, m_w_down, v_w_gate, v_w_up, v_w_down):
    weights = dict(zip(NAMES, (w_gate, w_up, w_down), strict=True))

    def take(so_far, sequence):
        h, by_y = sequence
        _, back = jax.vjp(lambda w: stack(w, h), weights)
        return jax.tree.map(lambda total, term: total + term.astype(jnp.float32), so_far, back(by_y)[0]), None

    none_yet = {name: jnp.zeros(w.shape, jnp.float32) for name, w in weights.items()}
    by_weights, _ = lax.scan(take, none_yet, (x, dy))
    gradients = [by_weights[name].astype(jnp.bfloat16).astype(jnp.float32) for name in NAMES]
    gradients = clipped(gradients, sum(jnp.sum(g * g) for g in gradients), sum(g.size for g in gradients))
    new = [
        adamw(w.astype(jnp.float32), m, v, g)
        for w, m, v, g in zip((w_gate, w_up, w_down), (m_w_gate, m_w_up, m_w_down), (v_w_gate, v_w_up, v_w_down), gradients, strict=True)
    ]
    return tuple(one[which] for which in range(3) for one in new)
```

```python
import functools

import jax
import jax.numpy as jnp
from jax import lax
from jax.experimental import pallas as pl
from jax.experimental.pallas import tpu as pltpu
from jax.sharding import PartitionSpec as P

NAMES = ("w_gate", "w_up", "w_down")
MESH = pl.DeviceIdType.MESH
F32, BF16 = jnp.float32, jnp.bfloat16


def matmul(a, w):
    return jnp.dot(a, w, preferred_element_type=F32).astype(BF16)


def normed(h):
    wide = h.astype(F32)
    scale = lax.rsqrt(jnp.mean(wide**2, -1, keepdims=True) + 1e-6)
    return (wide * scale).astype(BF16)


def layer(h, w):
    a = normed(h)
    gate = jnp.dot(a, w["w_gate"], preferred_element_type=F32)
    up = jnp.dot(a, w["w_up"], preferred_element_type=F32)
    return h + matmul((jax.nn.silu(gate) * up).astype(BF16), w["w_down"])


def stack(weights, h):
    for number in range(weights["w_gate"].shape[0]):
        h = layer(h, {name: w[number] for name, w in weights.items()})
    return h


def update_kernel(n, layers, count, *refs):
    ssq, g, w, m, v = refs[0], refs[1:4], refs[4:7], refs[7:10], refs[10:13]
    nw, nm, nv = refs[13:16], refs[16:19], refs[19:22]
    gs, ws, ms, vs = refs[22:25], refs[25:28], refs[28:31], refs[31:34]
    slots, load_sem, store_sem, own_sem, ssq_send, ssq_recv, send_sem, recv_sem = refs[34:]
    me = lax.axis_index("dp")
    right, left = lax.rem(me + 1, n), lax.rem(me + n - 1, n)
    blocks = [(i, l) for l in range(layers) for i in range(3)]
    rows = [r.shape[1] for r in g]

    loads = {}
    for k, (i, l) in enumerate(blocks):
        own = pl.ds(pl.multiple_of(me * rows[i], rows[i]), rows[i])
        pairs = ((g[i].at[l], gs[i].at[l]), (w[i].at[l, own], ws[i].at[l]), (m[i].at[l], ms[i].at[l]), (v[i].at[l], vs[i].at[l]))
        loads[k] = [pltpu.make_async_copy(src, dst, load_sem.at[k, j]) for j, (src, dst) in enumerate(pairs)]
        for copy in loads[k]:
            copy.start()

    barrier = pltpu.get_barrier_semaphore()
    for d in range(1, n):
        pl.semaphore_signal(barrier, inc=1, device_id={"dp": lax.rem(me + d, n)}, device_id_type=MESH)
    pl.semaphore_wait(barrier, n - 1)

    sums = [
        pltpu.make_async_remote_copy(
            src_ref=ssq, dst_ref=slots.at[d], send_sem=ssq_send.at[d], recv_sem=ssq_recv.at[d],
            device_id={"dp": lax.rem(me + d, n)}, device_id_type=MESH,
        )
        for d in range(1, n)
    ]
    for copy in sums:
        copy.start()
    total = ssq[...]
    for d, copy in enumerate(sums, 1):
        copy.wait()
        total = total + slots[d]
    total = jnp.sum(jnp.sum(total, axis=1, keepdims=True), axis=0, keepdims=True)
    factor = jnp.minimum(1.0, 0.5 * lax.rsqrt(total / count + 1e-30))

    def piece(ref, i, l, owner, way):
        half = rows[i] // 2
        return ref.at[l, pl.ds(pl.multiple_of(owner * rows[i] + way * half, half), half)]

    def hop(k, way, step, first):
        i, l = blocks[k]
        owner = lax.rem(me + (n - step if way == 0 else step), n)
        half = rows[i] // 2
        src = ws[i].at[l, pl.ds(way * half, half)] if first else piece(nw[i], i, l, owner, way)
        return pltpu.make_async_remote_copy(
            src_ref=src, dst_ref=piece(nw[i], i, l, owner, way), send_sem=send_sem.at[way, k, step], recv_sem=recv_sem.at[way, k, step],
            device_id={"dp": (right, left)[way]}, device_id_type=MESH,
        )

    stores = []
    for k, (i, l) in enumerate(blocks):
        for copy in loads[k]:
            copy.wait()
        tile = 32

        def body(t, _, i=i, l=l, tile=tile):
            at = (l, pl.ds(pl.multiple_of(t * tile, tile), tile))
            grad = gs[i][at].astype(F32) * factor
            wide = ws[i][at].astype(F32)
            new_m = 0.9 * ms[i][at] + 0.1 * grad
            new_v = 0.95 * vs[i][at] + 0.05 * grad * grad
            ms[i][at] = new_m
            vs[i][at] = new_v
            step = new_m * lax.rsqrt(new_v + 1e-8) + 0.1 * wide
            ws[i][at] = (wide - 0.02 * step).astype(BF16)
            return 0

        lax.fori_loop(0, rows[i] // tile, body, 0)
        for way in range(2):
            hop(k, way, 0, True).start()
        own = pl.ds(pl.multiple_of(me * rows[i], rows[i]), rows[i])
        pairs = ((ws[i].at[l], nw[i].at[l, own]), (ms[i].at[l], nm[i].at[l]), (vs[i].at[l], nv[i].at[l]))
        for j, (src, dst) in enumerate(pairs):
            stores.append(pltpu.make_async_copy(src, dst, store_sem.at[k, j]))
            stores[-1].start()

    for step in range(1, n):
        for k in range(len(blocks)):
            for way in range(2):
                hop(k, way, step - 1, False).wait_recv()
                if step < n - 1:
                    hop(k, way, step, False).start()
    for step in range(n - 1):
        for k in range(len(blocks)):
            for way in range(2):
                hop(k, way, step, step == 0).wait_send()
    for copy in stores:
        copy.wait()


def update(n, ssq, g, w, m, v):
    layers = w[0].shape[0]
    count = float(sum(t.size for t in w))
    blocks = 3 * layers
    anywhere = pl.BlockSpec(memory_space=pl.ANY)
    outs = pl.pallas_call(
        functools.partial(update_kernel, n, layers, count),
        out_shape=[jax.ShapeDtypeStruct(t.shape, t.dtype) for t in (*w, *m, *v)],
        in_specs=[pl.BlockSpec(memory_space=pltpu.VMEM)] + [anywhere] * 12,
        out_specs=[anywhere] * 9,
        scratch_shapes=[pltpu.VMEM(t.shape, t.dtype) for t in (*g, *g, *m, *v)]
        + [
            pltpu.VMEM((n, *ssq.shape), F32),
            pltpu.SemaphoreType.DMA((blocks, 4)),
            pltpu.SemaphoreType.DMA((blocks, 3)),
            pltpu.SemaphoreType.DMA((1,)),
            pltpu.SemaphoreType.DMA((n,)),
            pltpu.SemaphoreType.DMA((n,)),
            pltpu.SemaphoreType.DMA((2, blocks, n - 1)),
            pltpu.SemaphoreType.DMA((2, blocks, n - 1)),
        ],
        compiler_params=pltpu.CompilerParams(collective_id=1, has_side_effects=True, vmem_limit_bytes=40 * 2**20),
        name="update",
    )(ssq, *g, *w, *m, *v)
    return tuple(outs)


def solution(mesh):
    n = mesh.shape["dp"]

    def device(x, dy, *arrays):
        w, m, v = (arrays[i : i + 3] for i in (0, 3, 6))
        _, back = jax.vjp(lambda w: stack(w, x[0]), dict(zip(NAMES, w, strict=True)))
        by_weights = back(dy[0])[0]
        g = [lax.psum_scatter(by_weights[name], "dp", scatter_dimension=1, tiled=True) for name in NAMES]
        ssq = sum(jnp.sum(jnp.square(t.astype(F32))) for t in g)
        ssq = jnp.zeros((8, 128), F32).at[0, 0].set(ssq)
        return update(n, ssq, g, w, m, v)

    whole, part = P(None, None, None), P(None, "dp", None)
    return jax.shard_map(
        device,
        mesh=mesh,
        in_specs=(P(("rep", "dp")), P(("rep", "dp"))) + (whole,) * 3 + (part,) * 6,
        out_specs=(P("rep"),) * 3 + (P("rep", "dp"),) * 6,
        check_vma=False,
    )
```

```python
import functools

import jax
import jax.numpy as jnp
from jax import lax
from jax.experimental import pallas as pl
from jax.experimental.pallas import tpu as pltpu
from jax.sharding import PartitionSpec as P

MESH = pl.DeviceIdType.MESH
STARTS = (4, 8, 12, 16, 16, 16, 20, 22, 24, 26, 26, 26)
F32, BF16 = jnp.float32, jnp.bfloat16


def unit_scale(wide):
    return lax.rsqrt(jnp.mean(wide * wide, -1, keepdims=True) + 1e-6)


def nn(a, b):
    return lax.dot_general(a, b, (((1,), (0,)), ((), ())), preferred_element_type=F32)


def nt(a, b):
    return lax.dot_general(a, b, (((1,), (1,)), ((), ())), preferred_element_type=F32)


def gradients_kernel(n, *refs):
    x, dy, wg, wu, wd, og, ou, od, ossq = refs[:9]
    h, a, at, d, dt, acc, wgb, wub, wdb, act, dg, du, gg, gu, gd, rgu, rd = refs[9:26]
    wsem, xsem, osem, send_sem, recv_sem, credit = refs[26:]
    me = lax.axis_index("dp")
    right, left = lax.rem(me + 1, n), lax.rem(me + n - 1, n)
    tokens, width = h.shape
    hidden = wg.shape[2]
    chunk = act.shape[1]
    chunks = hidden // chunk
    tile = tokens // 4
    rows, deep = og.shape[1], od.shape[1] // 2
    wide_cols, half_cols = rgu.shape[-1], rd.shape[-1]

    def tokens_at(i):
        return pl.ds(pl.multiple_of(i * tile, tile), tile)

    def chunk_of(t):
        number = jnp.where(lax.div(t, chunks) == 1, 1, 0)
        cols = pl.ds(pl.multiple_of(lax.rem(t, chunks) * chunk, chunk), chunk)
        slot = lax.rem(t, 2)
        return [
            pltpu.make_async_copy(wg.at[number, :, cols], wgb.at[slot], wsem.at[slot, 0]),
            pltpu.make_async_copy(wu.at[number, :, cols], wub.at[slot], wsem.at[slot, 1]),
            pltpu.make_async_copy(wd.at[number, cols, :], wdb.at[slot], wsem.at[slot, 2]),
        ]

    def next_chunk(t, last):
        for copy in chunk_of(t):
            copy.wait()

        @pl.when(t < last)
        def _():
            for copy in chunk_of(t + 1):
                copy.start()

    load_x = pltpu.make_async_copy(x, h, xsem.at[0])
    load_dy = pltpu.make_async_copy(dy, d, xsem.at[1])
    load_x.start()
    for copy in chunk_of(0):
        copy.start()
    load_dy.start()
    barrier = pltpu.get_barrier_semaphore()
    for neighbour in (left, right):
        pl.semaphore_signal(barrier, inc=1, device_id={"dp": neighbour}, device_id_type=MESH)
    load_x.wait()

    def norm_all():
        def body(i, _):
            wide = h[tokens_at(i), :].astype(F32)
            a[tokens_at(i), :] = (wide * unit_scale(wide)).astype(BF16)
            return 0

        lax.fori_loop(0, 4, body, 0)

    def turn(src, dst, i, size):
        part = pl.ds(pl.multiple_of(i * size, size), size)
        dst[:, part] = src[part, :].T

    norm_all()
    acc[...] = jnp.zeros_like(acc)
    load_dy.wait()

    def forward(t, _):
        next_chunk(t, 3 * chunks - 1)
        slot = lax.rem(t, 2)
        turn(d, dt, t, tokens // chunks)
        for i in range(4):
            part = pl.ds(i * tile, tile)
            gate = nn(a[part, :], wgb[slot])
            up = nn(a[part, :], wub[slot])
            acc[part, :] += nn((gate * jax.nn.sigmoid(gate) * up).astype(BF16), wdb[slot])
        return 0

    lax.fori_loop(0, chunks, forward, 0)

    def between(i, _):
        out = (h[tokens_at(i), :].astype(F32) + acc[tokens_at(i), :].astype(BF16).astype(F32)).astype(BF16)
        h[tokens_at(i), :] = out
        wide = out.astype(F32)
        a[tokens_at(i), :] = (wide * unit_scale(wide)).astype(BF16)
        acc[tokens_at(i), :] = jnp.zeros((tile, width), F32)
        turn(a, at, i, tile)
        return 0

    lax.fori_loop(0, 4, between, 0)
    ossq[...] = jnp.zeros_like(ossq)
    pl.semaphore_wait(barrier, 2)

    def block(kind, way, j, owner):
        number = jnp.where(j < 6, 1, 0)
        part = lax.rem(j, 6)
        if kind == 0:
            at_rows = pl.ds(pl.multiple_of(owner * rows, rows), rows)
            at_cols = pl.ds(pl.multiple_of(part * wide_cols, wide_cols), wide_cols)
            return (gg, gu)[way].at[number, at_rows, at_cols]
        at_rows = pl.ds(pl.multiple_of(owner * 2 * deep + (part - 4) * deep, deep), deep)
        return gd.at[number, at_rows, pl.ds(way * half_cols, half_cols)]

    def landing(kind, way, j, s):
        part = lax.rem(j, 6)
        return rgu.at[way, part, s] if kind == 0 else rd.at[way, part - 4, s]

    def hop(kind, way, lane, j, s):
        owner = lax.rem(me + (n - 1 - s if way == 0 else 1 + s), n)
        return pltpu.make_async_remote_copy(
            src_ref=block(kind, way, j, owner), dst_ref=landing(kind, way, j, s),
            send_sem=send_sem.at[way, lane], recv_sem=recv_sem.at[way, lax.rem(j, 6), s],
            device_id={"dp": (right, left)[way]}, device_id_type=MESH,
        )

    def serve(kind, lane, j, s, valid):
        @pl.when(jnp.logical_and(valid, s == 0))
        def _():
            @pl.when(j >= 6)
            def _():
                for way in range(2):
                    pl.semaphore_wait(credit.at[way, lane], 1)

            for way in range(2):
                hop(kind, way, lane, j, s).start()

        @pl.when(jnp.logical_and(valid, s > 0))
        def _():
            for way in range(2):
                before = hop(kind, way, lane, j, s - 1)
                before.wait_recv()
                owner = lax.rem(me + (2 * n - 1 - s if way == 0 else 1 + s), n)
                ref = block(kind, way, j, owner)
                ref[...] = (ref[...].astype(F32) + landing(kind, way, j, s - 1)[...].astype(F32)).astype(BF16)
                before.wait_send()

            @pl.when(s < n - 1)
            def _():
                for way in range(2):
                    hop(kind, way, lane, j, s).start()

            @pl.when(s == n - 1)
            def _():
                for way in range(2):
                    ended = block(kind, way, j, me)[...].astype(F32)
                    ended = (ended * ended).reshape(-1, 8, ended.shape[-1])
                    ended = jnp.sum(ended, axis=0)
                    for c in range(0, ended.shape[-1], 128):
                        ossq[...] += ended[:, c : c + 128]

                @pl.when(j < 6)
                def _():
                    for way in range(2):
                        pl.semaphore_signal(credit.at[way, lane], inc=1, device_id={"dp": (left, right)[way]}, device_id_type=MESH)

    def lane(which, step):
        first, second = STARTS[which], STARTS[which + 6]
        later = step >= second
        s = step - jnp.where(later, second, first)
        serve(0 if which < 4 else 1, which, jnp.where(later, which + 6, which), s, jnp.logical_and(s >= 0, s <= n - 1))

    def backward(number, count, rounds):
        t = chunks + count
        next_chunk(t, 3 * chunks - 1)
        slot = lax.rem(t, 2)
        cols = pl.ds(pl.multiple_of(lax.rem(count, chunks) * chunk, chunk), chunk)
        for i in range(4):
            part = pl.ds(i * tile, tile)
            gate = nn(a[part, :], wgb[slot])
            up = nn(a[part, :], wub[slot])
            back = nt(d[part, :], wdb[slot]).astype(BF16).astype(F32)
            sig = jax.nn.sigmoid(gate)
            silu = gate * sig
            act[part, :] = (silu * up).astype(BF16)
            by_up = (back * silu).astype(BF16)
            by_gate = (back * up * (sig + silu * (1.0 - sig))).astype(BF16)
            du[part, :] = by_up
            dg[part, :] = by_gate
            if number == 1:
                acc[part, :] += nt(by_gate, wgb[slot]) + nt(by_up, wub[slot])
            rounds(i)
        gg[number, :, cols] = nn(at[...], dg[...]).astype(BF16)
        rounds(4)
        gu[number, :, cols] = nn(at[...], du[...]).astype(BF16)
        rounds(5)
        gd[number, cols, :] = nn(dt[...], act[...]).T.astype(BF16)
        rounds(6)

    def last_layer(count, _):
        def rounds(place):
            if place not in (0, 4):
                which = {1: 0, 2: 1, 3: 2, 5: 0, 6: 1}[place]
                lane(which, 2 * count + (place > 3))
            if place == 6:
                lane(2, 2 * count + 1)

        backward(1, count, rounds)
        return 0

    lax.fori_loop(0, chunks, last_layer, 0)
    for which in (2, 3, 4, 5):
        lane(which, 2 * chunks)

    def through_norm(i, _):
        part = tokens_at(i)
        wide = h[part, :].astype(F32)
        scale = unit_scale(wide)
        by_a = acc[part, :].astype(BF16).astype(F32)
        by_scale = jnp.sum(by_a * wide, -1, keepdims=True) * (scale * scale * scale) * (-1.0 / width)
        by_h = (by_a * scale + by_scale * wide).astype(BF16)
        d[part, :] = (d[part, :].astype(F32) + by_h.astype(F32)).astype(BF16)
        return 0

    lax.fori_loop(0, 4, through_norm, 0)
    load_x = pltpu.make_async_copy(x, h, xsem.at[0])
    load_x.start()
    for which in (2, 3, 4, 5):
        lane(which, 2 * chunks + 1)
    load_x.wait()
    norm_all()

    def turn_both(i, _):
        turn(d, dt, i, tile)
        turn(a, at, i, tile)
        return 0

    lax.fori_loop(0, 4, turn_both, 0)

    def first_layer(count, _):
        def rounds(place):
            which = {0: 2, 1: 3, 2: 4, 3: 5, 5: 0, 6: 1}.get(place)
            if which is not None:
                lane(which, chunks + 2 + count)

        backward(0, count, rounds)
        return 0

    lax.fori_loop(chunks, 2 * chunks, first_layer, 0)

    def rest(step, _):
        for which in (0, 1, 2, 3, 4, 5):
            lane(which, step)
        return 0

    lax.fori_loop(3 * chunks + 2, 3 * chunks + 10, rest, 0)

    own = pl.ds(pl.multiple_of(me * rows, rows), rows)
    own_deep = pl.ds(pl.multiple_of(me * 2 * deep, 2 * deep), 2 * deep)
    outs = [
        pltpu.make_async_copy(gg.at[:, own, :], og, osem.at[0]),
        pltpu.make_async_copy(gu.at[:, own, :], ou, osem.at[1]),
        pltpu.make_async_copy(gd.at[:, own_deep, :], od, osem.at[2]),
    ]
    for copy in outs:
        copy.start()
    for copy in outs:
        copy.wait()


def gradients(n, x, dy, w):
    wg, wu, wd = w
    tokens, width = x.shape
    layers, _, hidden = wg.shape
    chunk, wide_cols = hidden // 8, hidden // 4
    rows, deep = width // n, hidden // n // 2
    anywhere = pl.BlockSpec(memory_space=pl.ANY)
    state = pltpu.VMEM((tokens, width), BF16)
    turned = pltpu.VMEM((width, tokens), BF16)
    hiddens = pltpu.VMEM((tokens, chunk), BF16)
    outs = pl.pallas_call(
        functools.partial(gradients_kernel, n),
        out_shape=[
            jax.ShapeDtypeStruct((layers, rows, hidden), BF16),
            jax.ShapeDtypeStruct((layers, rows, hidden), BF16),
            jax.ShapeDtypeStruct((layers, 2 * deep, width), BF16),
            jax.ShapeDtypeStruct((8, 128), F32),
        ],
        in_specs=[anywhere] * 5,
        out_specs=[anywhere] * 3 + [pl.BlockSpec(memory_space=pltpu.VMEM)],
        scratch_shapes=[
            state, state, turned, state, turned,
            pltpu.VMEM((tokens, width), F32),
            pltpu.VMEM((2, width, chunk), BF16),
            pltpu.VMEM((2, width, chunk), BF16),
            pltpu.VMEM((2, chunk, width), BF16),
            hiddens, hiddens, hiddens,
            pltpu.VMEM(wg.shape, BF16),
            pltpu.VMEM(wu.shape, BF16),
            pltpu.VMEM(wd.shape, BF16),
            pltpu.VMEM((2, 4, n - 1, rows, wide_cols), BF16),
            pltpu.VMEM((2, 2, n - 1, deep, width // 2), BF16),
            pltpu.SemaphoreType.DMA((2, 3)),
            pltpu.SemaphoreType.DMA((2,)),
            pltpu.SemaphoreType.DMA((3,)),
            pltpu.SemaphoreType.DMA((2, 6)),
            pltpu.SemaphoreType.DMA((2, 6, n - 1)),
            pltpu.SemaphoreType.REGULAR((2, 6)),
        ],
        compiler_params=pltpu.CompilerParams(collective_id=0, has_side_effects=True, vmem_limit_bytes=67_043_328),
        name="gradients",
    )(x, dy, *w)
    return outs[:3], outs[3]


def update_kernel(n, layers, count, *refs):
    ssq, g, w, m, v = refs[0], refs[1:4], refs[4:7], refs[7:10], refs[10:13]
    nw, nm, nv = refs[13:16], refs[16:19], refs[19:22]
    gs, ws, ms, vs = refs[22:25], refs[25:28], refs[28:31], refs[31:34]
    slots, load_sem, store_sem, own_sem, ssq_send, ssq_recv, send_sem, recv_sem = refs[34:]
    me = lax.axis_index("dp")
    right, left = lax.rem(me + 1, n), lax.rem(me + n - 1, n)
    blocks = [(i, l) for l in range(layers) for i in range(3)]
    rows = [r.shape[1] for r in g]

    loads = {}
    for k, (i, l) in enumerate(blocks):
        own = pl.ds(pl.multiple_of(me * rows[i], rows[i]), rows[i])
        pairs = ((g[i].at[l], gs[i].at[l]), (w[i].at[l, own], ws[i].at[l]), (m[i].at[l], ms[i].at[l]), (v[i].at[l], vs[i].at[l]))
        loads[k] = [pltpu.make_async_copy(src, dst, load_sem.at[k, j]) for j, (src, dst) in enumerate(pairs)]
        for copy in loads[k]:
            copy.start()

    barrier = pltpu.get_barrier_semaphore()
    for d in range(1, n):
        pl.semaphore_signal(barrier, inc=1, device_id={"dp": lax.rem(me + d, n)}, device_id_type=MESH)
    pl.semaphore_wait(barrier, n - 1)

    sums = [
        pltpu.make_async_remote_copy(
            src_ref=ssq, dst_ref=slots.at[d], send_sem=ssq_send.at[d], recv_sem=ssq_recv.at[d],
            device_id={"dp": lax.rem(me + d, n)}, device_id_type=MESH,
        )
        for d in range(1, n)
    ]
    for copy in sums:
        copy.start()
    total = ssq[...]
    for d, copy in enumerate(sums, 1):
        copy.wait()
        total = total + slots[d]
    total = jnp.sum(jnp.sum(total, axis=1, keepdims=True), axis=0, keepdims=True)
    factor = jnp.minimum(1.0, 0.5 * lax.rsqrt(total / count + 1e-30))

    def piece(ref, i, l, owner, way):
        half = rows[i] // 2
        return ref.at[l, pl.ds(pl.multiple_of(owner * rows[i] + way * half, half), half)]

    def hop(k, way, step, first):
        i, l = blocks[k]
        owner = lax.rem(me + (n - step if way == 0 else step), n)
        half = rows[i] // 2
        src = ws[i].at[l, pl.ds(way * half, half)] if first else piece(nw[i], i, l, owner, way)
        return pltpu.make_async_remote_copy(
            src_ref=src, dst_ref=piece(nw[i], i, l, owner, way), send_sem=send_sem.at[way, k, step], recv_sem=recv_sem.at[way, k, step],
            device_id={"dp": (right, left)[way]}, device_id_type=MESH,
        )

    stores = []
    for k, (i, l) in enumerate(blocks):
        for copy in loads[k]:
            copy.wait()
        tile = 32

        def body(t, _, i=i, l=l, tile=tile):
            at = (l, pl.ds(pl.multiple_of(t * tile, tile), tile))
            grad = gs[i][at].astype(F32) * factor
            wide = ws[i][at].astype(F32)
            new_m = 0.9 * ms[i][at] + 0.1 * grad
            new_v = 0.95 * vs[i][at] + 0.05 * grad * grad
            ms[i][at] = new_m
            vs[i][at] = new_v
            step = new_m * lax.rsqrt(new_v + 1e-8) + 0.1 * wide
            ws[i][at] = (wide - 0.02 * step).astype(BF16)
            return 0

        lax.fori_loop(0, rows[i] // tile, body, 0)
        for way in range(2):
            hop(k, way, 0, True).start()
        own = pl.ds(pl.multiple_of(me * rows[i], rows[i]), rows[i])
        pairs = ((ws[i].at[l], nw[i].at[l, own]), (ms[i].at[l], nm[i].at[l]), (vs[i].at[l], nv[i].at[l]))
        for j, (src, dst) in enumerate(pairs):
            stores.append(pltpu.make_async_copy(src, dst, store_sem.at[k, j]))
            stores[-1].start()

    for step in range(1, n):
        for k in range(len(blocks)):
            for way in range(2):
                hop(k, way, step - 1, False).wait_recv()
                if step < n - 1:
                    hop(k, way, step, False).start()
    for step in range(n - 1):
        for k in range(len(blocks)):
            for way in range(2):
                hop(k, way, step, step == 0).wait_send()
    for copy in stores:
        copy.wait()


def update(n, ssq, g, w, m, v):
    layers = w[0].shape[0]
    count = float(sum(t.size for t in w))
    blocks = 3 * layers
    anywhere = pl.BlockSpec(memory_space=pl.ANY)
    outs = pl.pallas_call(
        functools.partial(update_kernel, n, layers, count),
        out_shape=[jax.ShapeDtypeStruct(t.shape, t.dtype) for t in (*w, *m, *v)],
        in_specs=[pl.BlockSpec(memory_space=pltpu.VMEM)] + [anywhere] * 12,
        out_specs=[anywhere] * 9,
        scratch_shapes=[pltpu.VMEM(t.shape, t.dtype) for t in (*g, *g, *m, *v)]
        + [
            pltpu.VMEM((n, *ssq.shape), F32),
            pltpu.SemaphoreType.DMA((blocks, 4)),
            pltpu.SemaphoreType.DMA((blocks, 3)),
            pltpu.SemaphoreType.DMA((1,)),
            pltpu.SemaphoreType.DMA((n,)),
            pltpu.SemaphoreType.DMA((n,)),
            pltpu.SemaphoreType.DMA((2, blocks, n - 1)),
            pltpu.SemaphoreType.DMA((2, blocks, n - 1)),
        ],
        compiler_params=pltpu.CompilerParams(collective_id=1, has_side_effects=True, vmem_limit_bytes=40 * 2**20),
        name="update",
    )(ssq, *g, *w, *m, *v)
    return tuple(outs)


def solution(mesh):
    n = mesh.shape["dp"]

    def device(x, dy, *arrays):
        w, m, v = (arrays[i : i + 3] for i in (0, 3, 6))
        g, ssq = gradients(n, x[0], dy[0], w)
        return update(n, ssq, g, w, m, v)

    whole, part = P(None, None, None), P(None, "dp", None)
    return jax.shard_map(
        device,
        mesh=mesh,
        in_specs=(P(("rep", "dp")), P(("rep", "dp"))) + (whole,) * 3 + (part,) * 6,
        out_specs=(P("rep"),) * 3 + (P("rep", "dp"),) * 6,
        check_vma=False,
    )
```

```python
import functools

import jax
import jax.numpy as jnp
from jax import lax
from jax.experimental import pallas as pl
from jax.experimental.pallas import tpu as pltpu
from jax.sharding import PartitionSpec as P

MESH = pl.DeviceIdType.MESH
STARTS = (3, 6, 9, 12, 12, 12, 17, 18, 20, 22, 22, 22)
F32, BF16 = jnp.float32, jnp.bfloat16


def unit_scale(wide):
    return lax.rsqrt(jnp.mean(wide * wide, -1, keepdims=True) + 1e-6)


def nn(a, b):
    return lax.dot_general(a, b, (((1,), (0,)), ((), ())), preferred_element_type=F32)


def nt(a, b):
    return lax.dot_general(a, b, (((1,), (1,)), ((), ())), preferred_element_type=F32)


def gradients_kernel(n, *refs):
    x, dy, wg, wu, wd, og, ou, od, ossq = refs[:9]
    h, a, at, d, dt, acc, wgb, wub, wdb, act, dg, du, gg, gu, gd, rgu, rd = refs[9:26]
    wsem, xsem, osem, send_sem, recv_sem, credit = refs[26:]
    me = lax.axis_index("dp")
    right, left = lax.rem(me + 1, n), lax.rem(me + n - 1, n)
    tokens, width = h.shape
    hidden = wg.shape[2]
    chunk = act.shape[1]
    chunks = hidden // chunk
    tile = tokens // 4
    rows, deep = og.shape[1], od.shape[1] // 2
    wide_cols, half_cols = rgu.shape[-1], rd.shape[-1]

    def tokens_at(i):
        return pl.ds(pl.multiple_of(i * tile, tile), tile)

    def chunk_of(t):
        number = jnp.where(lax.div(t, chunks) == 1, 1, 0)
        cols = pl.ds(pl.multiple_of(lax.rem(t, chunks) * chunk, chunk), chunk)
        slot = lax.rem(t, 2)
        return [
            pltpu.make_async_copy(wg.at[number, :, cols], wgb.at[slot], wsem.at[slot, 0]),
            pltpu.make_async_copy(wu.at[number, :, cols], wub.at[slot], wsem.at[slot, 1]),
            pltpu.make_async_copy(wd.at[number, cols, :], wdb.at[slot], wsem.at[slot, 2]),
        ]

    def next_chunk(t, last):
        for copy in chunk_of(t):
            copy.wait()

        @pl.when(t < last)
        def _():
            for copy in chunk_of(t + 1):
                copy.start()

    load_x = pltpu.make_async_copy(x, h, xsem.at[0])
    load_dy = pltpu.make_async_copy(dy, d, xsem.at[1])
    load_x.start()
    for copy in chunk_of(0):
        copy.start()
    load_dy.start()
    barrier = pltpu.get_barrier_semaphore()
    for neighbour in (left, right):
        pl.semaphore_signal(barrier, inc=1, device_id={"dp": neighbour}, device_id_type=MESH)
    load_x.wait()

    def norm_all():
        def body(i, _):
            wide = h[tokens_at(i), :].astype(F32)
            a[tokens_at(i), :] = (wide * unit_scale(wide)).astype(BF16)
            return 0

        lax.fori_loop(0, 4, body, 0)

    def turn(src, dst, i, size):
        part = pl.ds(pl.multiple_of(i * size, size), size)
        dst[:, part] = src[part, :].T

    norm_all()
    acc[...] = jnp.zeros_like(acc)
    load_dy.wait()

    def forward(t, _):
        next_chunk(t, 3 * chunks - 1)
        slot = lax.rem(t, 2)
        turn(d, dt, t, tokens // chunks)
        for i in range(4):
            part = pl.ds(i * tile, tile)
            gate = nn(a[part, :], wgb[slot])
            up = nn(a[part, :], wub[slot])
            acc[part, :] += nn((gate * jax.nn.sigmoid(gate) * up).astype(BF16), wdb[slot])
        return 0

    lax.fori_loop(0, chunks, forward, 0)

    def between(i, _):
        out = (h[tokens_at(i), :].astype(F32) + acc[tokens_at(i), :].astype(BF16).astype(F32)).astype(BF16)
        h[tokens_at(i), :] = out
        wide = out.astype(F32)
        a[tokens_at(i), :] = (wide * unit_scale(wide)).astype(BF16)
        acc[tokens_at(i), :] = jnp.zeros((tile, width), F32)
        turn(a, at, i, tile)
        return 0

    lax.fori_loop(0, 4, between, 0)
    ossq[...] = jnp.zeros_like(ossq)
    pl.semaphore_wait(barrier, 2)

    def block(kind, way, j, owner):
        number = jnp.where(j < 6, 1, 0)
        part = lax.rem(j, 6)
        if kind == 0:
            at_rows = pl.ds(pl.multiple_of(owner * rows, rows), rows)
            at_cols = pl.ds(pl.multiple_of(part * wide_cols, wide_cols), wide_cols)
            return (gg, gu)[way].at[number, at_rows, at_cols]
        at_rows = pl.ds(pl.multiple_of(owner * 2 * deep + (part - 4) * deep, deep), deep)
        return gd.at[number, at_rows, pl.ds(way * half_cols, half_cols)]

    def landing(kind, way, j, s):
        part = lax.rem(j, 6)
        return rgu.at[way, part, s] if kind == 0 else rd.at[way, part - 4, s]

    def hop(kind, way, lane, j, s):
        owner = lax.rem(me + (n - 1 - s if way == 0 else 1 + s), n)
        return pltpu.make_async_remote_copy(
            src_ref=block(kind, way, j, owner), dst_ref=landing(kind, way, j, s),
            send_sem=send_sem.at[way, lane], recv_sem=recv_sem.at[way, lax.rem(j, 6), s],
            device_id={"dp": (right, left)[way]}, device_id_type=MESH,
        )

    def serve(kind, lane, j, s, valid):
        @pl.when(jnp.logical_and(valid, s == 0))
        def _():
            @pl.when(j >= 6)
            def _():
                for way in range(2):
                    pl.semaphore_wait(credit.at[way, lane], 1)

            for way in range(2):
                hop(kind, way, lane, j, s).start()

        @pl.when(jnp.logical_and(valid, s > 0))
        def _():
            for way in range(2):
                before = hop(kind, way, lane, j, s - 1)
                before.wait_recv()
                owner = lax.rem(me + (2 * n - 1 - s if way == 0 else 1 + s), n)
                ref = block(kind, way, j, owner)
                ref[...] = (ref[...].astype(F32) + landing(kind, way, j, s - 1)[...].astype(F32)).astype(BF16)
                before.wait_send()

            @pl.when(s < n - 1)
            def _():
                for way in range(2):
                    hop(kind, way, lane, j, s).start()

            @pl.when(s == n - 1)
            def _():
                for way in range(2):
                    ended = block(kind, way, j, me)[...].astype(F32)
                    ended = (ended * ended).reshape(-1, 8, ended.shape[-1])
                    ended = jnp.sum(ended, axis=0)
                    for c in range(0, ended.shape[-1], 128):
                        ossq[...] += ended[:, c : c + 128]

                @pl.when(j < 6)
                def _():
                    for way in range(2):
                        pl.semaphore_signal(credit.at[way, lane], inc=1, device_id={"dp": (left, right)[way]}, device_id_type=MESH)

    def lane(which, step, now=True):
        first, second = STARTS[which], STARTS[which + 6]
        later = step >= second
        s = step - jnp.where(later, second, first)
        due = jnp.logical_and(jnp.logical_and(s >= 0, s <= n - 1), now)
        serve(0 if which < 4 else 1, which, jnp.where(later, which + 6, which), s, due)

    def backward(number, count, rounds):
        t = chunks + count
        next_chunk(t, 3 * chunks - 1)
        slot = lax.rem(t, 2)
        cols = pl.ds(pl.multiple_of(lax.rem(count, chunks) * chunk, chunk), chunk)
        for i in range(4):
            part = pl.ds(i * tile, tile)
            gate = nn(a[part, :], wgb[slot])
            up = nn(a[part, :], wub[slot])
            back = nt(d[part, :], wdb[slot]).astype(BF16).astype(F32)
            sig = jax.nn.sigmoid(gate)
            silu = gate * sig
            act[part, :] = (silu * up).astype(BF16)
            by_up = (back * silu).astype(BF16)
            by_gate = (back * up * (sig + silu * (1.0 - sig))).astype(BF16)
            du[part, :] = by_up
            dg[part, :] = by_gate
            if number == 1:
                acc[part, :] += nt(by_gate, wgb[slot]) + nt(by_up, wub[slot])
            rounds(i)
        gg[number, :, cols] = nn(at[...], dg[...]).astype(BF16)
        rounds(4)
        gu[number, :, cols] = nn(at[...], du[...]).astype(BF16)
        rounds(5)
        gd[number, cols, :] = nn(dt[...], act[...]).T.astype(BF16)
        rounds(6)

    def last_layer(count, _):
        pair, odd = lax.div(count, 2), lax.rem(count, 2)

        def rounds(place):
            for which in (0, 1, 2):
                if place == 3:
                    lane(which, 3 * pair + 2 * odd)
                if place == 6:
                    lane(which, 3 * pair + 1, odd == 0)

        backward(1, count, rounds)
        return 0

    lax.fori_loop(0, chunks, last_layer, 0)
    middle = 3 * chunks // 2
    for which in (1, 2, 3, 4, 5):
        lane(which, middle)

    def through_norm(i, _):
        part = tokens_at(i)
        wide = h[part, :].astype(F32)
        scale = unit_scale(wide)
        by_a = acc[part, :].astype(BF16).astype(F32)
        by_scale = jnp.sum(by_a * wide, -1, keepdims=True) * (scale * scale * scale) * (-1.0 / width)
        by_h = (by_a * scale + by_scale * wide).astype(BF16)
        d[part, :] = (d[part, :].astype(F32) + by_h.astype(F32)).astype(BF16)
        return 0

    lax.fori_loop(0, 4, through_norm, 0)
    load_x = pltpu.make_async_copy(x, h, xsem.at[0])
    load_x.start()
    for which in (1, 2, 3, 4, 5):
        lane(which, middle + 1)
    load_x.wait()
    norm_all()

    def turn_both(i, _):
        turn(d, dt, i, tile)
        turn(a, at, i, tile)
        return 0

    lax.fori_loop(0, 4, turn_both, 0)

    def first_layer(count, _):
        def rounds(place):
            for which in {3: (2, 3, 4), 6: (5, 0, 1)}.get(place, ()):
                lane(which, middle + 2 + count - chunks)

        backward(0, count, rounds)
        return 0

    lax.fori_loop(chunks, 2 * chunks, first_layer, 0)

    def rest(step, _):
        for which in (0, 1, 2, 3, 4, 5):
            lane(which, step)
        return 0

    lax.fori_loop(middle + 2 + chunks, middle + 2 + chunks + n, rest, 0)

    own = pl.ds(pl.multiple_of(me * rows, rows), rows)
    own_deep = pl.ds(pl.multiple_of(me * 2 * deep, 2 * deep), 2 * deep)
    outs = [
        pltpu.make_async_copy(gg.at[:, own, :], og, osem.at[0]),
        pltpu.make_async_copy(gu.at[:, own, :], ou, osem.at[1]),
        pltpu.make_async_copy(gd.at[:, own_deep, :], od, osem.at[2]),
    ]
    for copy in outs:
        copy.start()
    for copy in outs:
        copy.wait()


def gradients(n, x, dy, w):
    wg, wu, wd = w
    tokens, width = x.shape
    layers, _, hidden = wg.shape
    chunk, wide_cols = hidden // 8, hidden // 4
    rows, deep = width // n, hidden // n // 2
    anywhere = pl.BlockSpec(memory_space=pl.ANY)
    state = pltpu.VMEM((tokens, width), BF16)
    turned = pltpu.VMEM((width, tokens), BF16)
    hiddens = pltpu.VMEM((tokens, chunk), BF16)
    outs = pl.pallas_call(
        functools.partial(gradients_kernel, n),
        out_shape=[
            jax.ShapeDtypeStruct((layers, rows, hidden), BF16),
            jax.ShapeDtypeStruct((layers, rows, hidden), BF16),
            jax.ShapeDtypeStruct((layers, 2 * deep, width), BF16),
            jax.ShapeDtypeStruct((8, 128), F32),
        ],
        in_specs=[anywhere] * 5,
        out_specs=[anywhere] * 3 + [pl.BlockSpec(memory_space=pltpu.VMEM)],
        scratch_shapes=[
            state, state, turned, state, turned,
            pltpu.VMEM((tokens, width), F32),
            pltpu.VMEM((2, width, chunk), BF16),
            pltpu.VMEM((2, width, chunk), BF16),
            pltpu.VMEM((2, chunk, width), BF16),
            hiddens, hiddens, hiddens,
            pltpu.VMEM(wg.shape, BF16),
            pltpu.VMEM(wu.shape, BF16),
            pltpu.VMEM(wd.shape, BF16),
            pltpu.VMEM((2, 4, n - 1, rows, wide_cols), BF16),
            pltpu.VMEM((2, 2, n - 1, deep, width // 2), BF16),
            pltpu.SemaphoreType.DMA((2, 3)),
            pltpu.SemaphoreType.DMA((2,)),
            pltpu.SemaphoreType.DMA((3,)),
            pltpu.SemaphoreType.DMA((2, 6)),
            pltpu.SemaphoreType.DMA((2, 6, n - 1)),
            pltpu.SemaphoreType.REGULAR((2, 6)),
        ],
        compiler_params=pltpu.CompilerParams(collective_id=0, has_side_effects=True, vmem_limit_bytes=67_043_328),
        name="gradients",
    )(x, dy, *w)
    return outs[:3], outs[3]


def update_kernel(n, layers, count, *refs):
    ssq, g, w, m, v = refs[0], refs[1:4], refs[4:7], refs[7:10], refs[10:13]
    nw, nm, nv = refs[13:16], refs[16:19], refs[19:22]
    gs, ws, ms, vs = refs[22:25], refs[25:28], refs[28:31], refs[31:34]
    slots, load_sem, store_sem, own_sem, ssq_send, ssq_recv, send_sem, recv_sem = refs[34:]
    me = lax.axis_index("dp")
    right, left = lax.rem(me + 1, n), lax.rem(me + n - 1, n)
    blocks = [(i, l) for l in range(layers) for i in range(3)]
    rows = [r.shape[1] for r in g]

    loads = {}
    for k, (i, l) in enumerate(blocks):
        own = pl.ds(pl.multiple_of(me * rows[i], rows[i]), rows[i])
        pairs = ((g[i].at[l], gs[i].at[l]), (w[i].at[l, own], ws[i].at[l]), (m[i].at[l], ms[i].at[l]), (v[i].at[l], vs[i].at[l]))
        loads[k] = [pltpu.make_async_copy(src, dst, load_sem.at[k, j]) for j, (src, dst) in enumerate(pairs)]
        for copy in loads[k]:
            copy.start()

    barrier = pltpu.get_barrier_semaphore()
    for d in range(1, n):
        pl.semaphore_signal(barrier, inc=1, device_id={"dp": lax.rem(me + d, n)}, device_id_type=MESH)
    pl.semaphore_wait(barrier, n - 1)

    sums = [
        pltpu.make_async_remote_copy(
            src_ref=ssq, dst_ref=slots.at[d], send_sem=ssq_send.at[d], recv_sem=ssq_recv.at[d],
            device_id={"dp": lax.rem(me + d, n)}, device_id_type=MESH,
        )
        for d in range(1, n)
    ]
    for copy in sums:
        copy.start()
    total = ssq[...]
    for d, copy in enumerate(sums, 1):
        copy.wait()
        total = total + slots[d]
    total = jnp.sum(jnp.sum(total, axis=1, keepdims=True), axis=0, keepdims=True)
    factor = jnp.minimum(1.0, 0.5 * lax.rsqrt(total / count + 1e-30))

    def piece(ref, i, l, owner, way):
        half = rows[i] // 2
        return ref.at[l, pl.ds(pl.multiple_of(owner * rows[i] + way * half, half), half)]

    def hop(k, way, step, first):
        i, l = blocks[k]
        owner = lax.rem(me + (n - step if way == 0 else step), n)
        half = rows[i] // 2
        src = ws[i].at[l, pl.ds(way * half, half)] if first else piece(nw[i], i, l, owner, way)
        return pltpu.make_async_remote_copy(
            src_ref=src, dst_ref=piece(nw[i], i, l, owner, way), send_sem=send_sem.at[way, k, step], recv_sem=recv_sem.at[way, k, step],
            device_id={"dp": (right, left)[way]}, device_id_type=MESH,
        )

    stores = []
    for k, (i, l) in enumerate(blocks):
        for copy in loads[k]:
            copy.wait()
        tile = 32

        def body(t, _, i=i, l=l, tile=tile):
            at = (l, pl.ds(pl.multiple_of(t * tile, tile), tile))
            grad = gs[i][at].astype(F32) * factor
            wide = ws[i][at].astype(F32)
            new_m = 0.9 * ms[i][at] + 0.1 * grad
            new_v = 0.95 * vs[i][at] + 0.05 * grad * grad
            ms[i][at] = new_m
            vs[i][at] = new_v
            step = new_m * lax.rsqrt(new_v + 1e-8) + 0.1 * wide
            ws[i][at] = (wide - 0.02 * step).astype(BF16)
            return 0

        lax.fori_loop(0, rows[i] // tile, body, 0)
        for way in range(2):
            hop(k, way, 0, True).start()
        own = pl.ds(pl.multiple_of(me * rows[i], rows[i]), rows[i])
        pairs = ((ws[i].at[l], nw[i].at[l, own]), (ms[i].at[l], nm[i].at[l]), (vs[i].at[l], nv[i].at[l]))
        for j, (src, dst) in enumerate(pairs):
            stores.append(pltpu.make_async_copy(src, dst, store_sem.at[k, j]))
            stores[-1].start()

    for step in range(1, n):
        for k in range(len(blocks)):
            for way in range(2):
                hop(k, way, step - 1, False).wait_recv()
                if step < n - 1:
                    hop(k, way, step, False).start()
    for step in range(n - 1):
        for k in range(len(blocks)):
            for way in range(2):
                hop(k, way, step, step == 0).wait_send()
    for copy in stores:
        copy.wait()


def update(n, ssq, g, w, m, v):
    layers = w[0].shape[0]
    count = float(sum(t.size for t in w))
    blocks = 3 * layers
    anywhere = pl.BlockSpec(memory_space=pl.ANY)
    g, w, m, v = ([pltpu.with_memory_space_constraint(t, pltpu.HBM) for t in ts] for ts in (g, w, m, v))
    outs = pl.pallas_call(
        functools.partial(update_kernel, n, layers, count),
        out_shape=[jax.ShapeDtypeStruct(t.shape, t.dtype) for t in (*w, *m, *v)],
        in_specs=[pl.BlockSpec(memory_space=pltpu.VMEM)] + [pl.BlockSpec(memory_space=pltpu.HBM)] * 12,
        out_specs=[anywhere] * 9,
        scratch_shapes=[pltpu.VMEM(t.shape, t.dtype) for t in (*g, *g, *m, *v)]
        + [
            pltpu.VMEM((n, *ssq.shape), F32),
            pltpu.SemaphoreType.DMA((blocks, 4)),
            pltpu.SemaphoreType.DMA((blocks, 3)),
            pltpu.SemaphoreType.DMA((1,)),
            pltpu.SemaphoreType.DMA((n,)),
            pltpu.SemaphoreType.DMA((n,)),
            pltpu.SemaphoreType.DMA((2, blocks, n - 1)),
            pltpu.SemaphoreType.DMA((2, blocks, n - 1)),
        ],
        compiler_params=pltpu.CompilerParams(collective_id=1, has_side_effects=True, vmem_limit_bytes=16 * 2**20),
        name="update",
    )(ssq, *g, *w, *m, *v)
    return tuple(outs)


def settle_kernel(*refs):
    *arrays, sems = refs
    half = len(arrays) // 2
    copies = [pltpu.make_async_copy(arrays[k], arrays[half + k], sems.at[k]) for k in range(half)]
    for copy in copies:
        copy.start()
    for copy in copies:
        copy.wait()


def settle(results):
    anywhere = pl.BlockSpec(memory_space=pl.ANY)
    return pl.pallas_call(
        settle_kernel,
        out_shape=[jax.ShapeDtypeStruct(t.shape, t.dtype) for t in results],
        in_specs=[anywhere] * len(results),
        out_specs=[anywhere] * len(results),
        scratch_shapes=[pltpu.SemaphoreType.DMA((len(results),))],
        compiler_params=pltpu.CompilerParams(vmem_limit_bytes=2**20),
        name="settle",
    )(*results)


def solution(mesh):
    n = mesh.shape["dp"]

    def device(x, dy, *arrays):
        w, m, v = (arrays[i : i + 3] for i in (0, 3, 6))
        g, ssq = gradients(n, x[0], dy[0], w)
        return tuple(settle(update(n, ssq, g, w, m, v)))

    whole, part = P(None, None, None), P(None, "dp", None)
    return jax.shard_map(
        device,
        mesh=mesh,
        in_specs=(P(("rep", "dp")), P(("rep", "dp"))) + (whole,) * 3 + (part,) * 6,
        out_specs=(P("rep"),) * 3 + (P("rep", "dp"),) * 6,
        check_vma=False,
    )
```

```python
import functools

import jax
import jax.numpy as jnp
from jax import lax
from jax.experimental import pallas as pl
from jax.experimental.pallas import tpu as pltpu
from jax.sharding import PartitionSpec as P

MESH = pl.DeviceIdType.MESH
STARTS = (1, 3, 5, 7, 7, 7, 12, 14, 16, 19, 19, 19)
F32, BF16 = jnp.float32, jnp.bfloat16


def unit_scale(wide):
    return lax.rsqrt(jnp.mean(wide * wide, -1, keepdims=True) + 1e-6)


def nn(a, b):
    return lax.dot_general(a, b, (((1,), (0,)), ((), ())), preferred_element_type=F32)


def nt(a, b):
    return lax.dot_general(a, b, (((1,), (1,)), ((), ())), preferred_element_type=F32)


def gradients_kernel(n, *refs):
    x, dy, wg, wu, wd, og, ou, od, ossq, spill = refs[:10]
    h, a, at, d, dt, acc, wgb, wub, wdb, act, dg, du, gg, gu, gd, rgu, rd = refs[10:27]
    wsem, xsem, osem, send_sem, recv_sem, credit, spill_sem = refs[27:]
    me = lax.axis_index("dp")
    right, left = lax.rem(me + 1, n), lax.rem(me + n - 1, n)
    tokens, width = h.shape
    hidden = wg.shape[2]
    chunk = act.shape[1]
    chunks = hidden // chunk
    tile = tokens // 4
    rows, deep = og.shape[1], od.shape[1] // 2
    wide_cols, half_cols = rgu.shape[-1], rd.shape[-1]

    def tokens_at(i):
        return pl.ds(pl.multiple_of(i * tile, tile), tile)

    def chunk_of(t):
        number = jnp.where(jnp.logical_or(lax.div(t, chunks) == 1, lax.div(t, chunks) == 2), 1, 0)
        cols = pl.ds(pl.multiple_of(lax.rem(t, chunks) * chunk, chunk), chunk)
        slot = lax.rem(t, 2)
        return [
            pltpu.make_async_copy(wg.at[number, :, cols], wgb.at[slot], wsem.at[slot, 0]),
            pltpu.make_async_copy(wu.at[number, :, cols], wub.at[slot], wsem.at[slot, 1]),
            pltpu.make_async_copy(wd.at[number, cols, :], wdb.at[slot], wsem.at[slot, 2]),
        ]

    def next_chunk(t, last):
        for copy in chunk_of(t):
            copy.wait()

        @pl.when(t < last)
        def _():
            for copy in chunk_of(t + 1):
                copy.start()

    load_x = pltpu.make_async_copy(x, h, xsem.at[0])
    load_dy = pltpu.make_async_copy(dy, d, xsem.at[1])
    load_x.start()
    for copy in chunk_of(0):
        copy.start()
    load_dy.start()
    barrier = pltpu.get_barrier_semaphore()
    for neighbour in (left, right):
        pl.semaphore_signal(barrier, inc=1, device_id={"dp": neighbour}, device_id_type=MESH)
    load_x.wait()

    def norm_all():
        def body(i, _):
            wide = h[tokens_at(i), :].astype(F32)
            a[tokens_at(i), :] = (wide * unit_scale(wide)).astype(BF16)
            return 0

        lax.fori_loop(0, 4, body, 0)

    def turn(src, dst, i, size):
        part = pl.ds(pl.multiple_of(i * size, size), size)
        dst[:, part] = src[part, :].T

    norm_all()
    acc[...] = jnp.zeros_like(acc)
    load_dy.wait()

    def forward(t, _):
        next_chunk(t, 4 * chunks - 1)
        slot = lax.rem(t, 2)
        turn(d, dt, t, tokens // chunks)
        for i in range(4):
            part = pl.ds(i * tile, tile)
            gate = nn(a[part, :], wgb[slot])
            up = nn(a[part, :], wub[slot])
            acc[part, :] += nn((gate * jax.nn.sigmoid(gate) * up).astype(BF16), wdb[slot])
        return 0

    lax.fori_loop(0, chunks, forward, 0)

    def between(i, _):
        out = (h[tokens_at(i), :].astype(F32) + acc[tokens_at(i), :].astype(BF16).astype(F32)).astype(BF16)
        h[tokens_at(i), :] = out
        wide = out.astype(F32)
        a[tokens_at(i), :] = (wide * unit_scale(wide)).astype(BF16)
        acc[tokens_at(i), :] = jnp.zeros((tile, width), F32)
        turn(a, at, i, tile)
        return 0

    lax.fori_loop(0, 4, between, 0)
    ossq[...] = jnp.zeros_like(ossq)
    pl.semaphore_wait(barrier, 2)

    def block(kind, way, j, owner):
        number = jnp.where(j < 6, 1, 0)
        part = lax.rem(j, 6)
        if kind == 0:
            at_rows = pl.ds(pl.multiple_of(owner * rows, rows), rows)
            at_cols = pl.ds(pl.multiple_of(part * wide_cols, wide_cols), wide_cols)
            return (gg, gu)[way].at[number, at_rows, at_cols]
        at_rows = pl.ds(pl.multiple_of(owner * 2 * deep + (part - 4) * deep, deep), deep)
        return gd.at[number, at_rows, pl.ds(way * half_cols, half_cols)]

    def landing(kind, way, j, s):
        part = lax.rem(j, 6)
        return rgu.at[way, part, s] if kind == 0 else rd.at[way, part - 4, s]

    def hop(kind, way, lane, j, s):
        owner = lax.rem(me + (n - 1 - s if way == 0 else 1 + s), n)
        return pltpu.make_async_remote_copy(
            src_ref=block(kind, way, j, owner), dst_ref=landing(kind, way, j, s),
            send_sem=send_sem.at[way, lane], recv_sem=recv_sem.at[way, lax.rem(j, 6), s],
            device_id={"dp": (right, left)[way]}, device_id_type=MESH,
        )

    def serve(kind, lane, j, s, valid):
        @pl.when(jnp.logical_and(valid, s == 0))
        def _():
            @pl.when(j >= 6)
            def _():
                for way in range(2):
                    pl.semaphore_wait(credit.at[way, lane], 1)

            for way in range(2):
                hop(kind, way, lane, j, s).start()

        @pl.when(jnp.logical_and(valid, s > 0))
        def _():
            for way in range(2):
                before = hop(kind, way, lane, j, s - 1)
                before.wait_recv()
                owner = lax.rem(me + (2 * n - 1 - s if way == 0 else 1 + s), n)
                ref = block(kind, way, j, owner)
                ref[...] = (ref[...].astype(F32) + landing(kind, way, j, s - 1)[...].astype(F32)).astype(BF16)
                before.wait_send()

            @pl.when(s < n - 1)
            def _():
                for way in range(2):
                    hop(kind, way, lane, j, s).start()

            @pl.when(s == n - 1)
            def _():
                for way in range(2):
                    ended = block(kind, way, j, me)[...].astype(F32)
                    ended = (ended * ended).reshape(-1, 8, ended.shape[-1])
                    ended = jnp.sum(ended, axis=0)
                    for c in range(0, ended.shape[-1], 128):
                        ossq[...] += ended[:, c : c + 128]

                @pl.when(j < 6)
                def _():
                    for way in range(2):
                        pl.semaphore_signal(credit.at[way, lane], inc=1, device_id={"dp": (left, right)[way]}, device_id_type=MESH)

    def lane(which, step, now=True):
        first, second = STARTS[which], STARTS[which + 6]
        later = step >= second
        s = step - jnp.where(later, second, first)
        due = jnp.logical_and(jnp.logical_and(s >= 0, s <= n - 1), now)
        serve(0 if which < 4 else 1, which, jnp.where(later, which + 6, which), s, due)

    def kept(count):
        slot = lax.rem(count, 2)
        return [pltpu.make_async_copy(ref.at[slot], spill.at[k, count], spill_sem.at[k, slot]) for k, ref in enumerate((dg, du))]

    def again(count):
        slot = lax.rem(count, 2)
        return [pltpu.make_async_copy(spill.at[k, count], ref.at[slot], spill_sem.at[k, slot]) for k, ref in enumerate((dg, du))]

    def backward(number, count, rounds):
        t = jnp.where(count < chunks, chunks, 2 * chunks) + count
        next_chunk(t, 4 * chunks - 1)
        slot = lax.rem(t, 2)
        cols = pl.ds(pl.multiple_of(lax.rem(count, chunks) * chunk, chunk), chunk)
        if number == 1:

            @pl.when(count >= 2)
            def _():
                for copy in kept(count - 2):
                    copy.wait()

        for i in range(4):
            part = pl.ds(i * tile, tile)
            gate = nn(a[part, :], wgb[slot])
            up = nn(a[part, :], wub[slot])
            back = nt(d[part, :], wdb[slot]).astype(BF16).astype(F32)
            sig = jax.nn.sigmoid(gate)
            silu = gate * sig
            act[part, :] = (silu * up).astype(BF16)
            by_up = (back * silu).astype(BF16)
            by_gate = (back * up * (sig + silu * (1.0 - sig))).astype(BF16)
            du[slot, part, :] = by_up
            dg[slot, part, :] = by_gate
            rounds(i)
        gg[number, :, cols] = nn(at[...], dg[slot]).astype(BF16)
        rounds(4)
        gu[number, :, cols] = nn(at[...], du[slot]).astype(BF16)
        rounds(5)
        gd[number, cols, :] = nn(dt[...], act[...]).T.astype(BF16)
        if number == 1:
            for copy in kept(count):
                copy.start()
        rounds(6)

    def last_layer(count, _):
        def rounds(place):
            if place == 6:
                for which in (0, 1, 2):
                    lane(which, count)

        backward(1, count, rounds)
        return 0

    lax.fori_loop(0, chunks, last_layer, 0)
    for which in (3, 4, 5):
        lane(which, chunks - 1)

    for count in (chunks - 2, chunks - 1):
        for copy in kept(count):
            copy.wait()
    for copy in again(0):
        copy.start()

    def state_half(half, _):
        def state(count, _):
            next_chunk(2 * chunks + count, 4 * chunks - 1)
            slot = lax.rem(count, 2)
            for copy in again(count):
                copy.wait()

            @pl.when(count < chunks - 1)
            def _():
                for copy in again(count + 1):
                    copy.start()

            for i in range(4):
                part = pl.ds(i * tile, tile)
                acc[part, :] += nt(dg[slot, part, :], wgb[slot]) + nt(du[slot, part, :], wub[slot])
            return 0

        lax.fori_loop(half * (chunks // 2), (half + 1) * (chunks // 2), state, 0)
        for which in (0, 1, 2, 3, 4, 5):
            lane(which, chunks + half)
        return 0

    lax.fori_loop(0, 2, state_half, 0)

    def through_norm(i, _):
        part = tokens_at(i)
        wide = h[part, :].astype(F32)
        scale = unit_scale(wide)
        by_a = acc[part, :].astype(BF16).astype(F32)
        by_scale = jnp.sum(by_a * wide, -1, keepdims=True) * (scale * scale * scale) * (-1.0 / width)
        by_h = (by_a * scale + by_scale * wide).astype(BF16)
        d[part, :] = (d[part, :].astype(F32) + by_h.astype(F32)).astype(BF16)
        return 0

    lax.fori_loop(0, 4, through_norm, 0)
    load_x = pltpu.make_async_copy(x, h, xsem.at[0])
    load_x.start()
    for which in (1, 2, 3, 4, 5):
        lane(which, chunks + 2)
    load_x.wait()
    norm_all()

    def turn_both(i, _):
        turn(d, dt, i, tile)
        turn(a, at, i, tile)
        return 0

    lax.fori_loop(0, 4, turn_both, 0)

    def first_layer(count, _):
        def rounds(place):
            for which in {3: (3, 4, 5), 6: (0, 1, 2)}.get(place, ()):
                lane(which, 3 + count)

        backward(0, count, rounds)
        return 0

    lax.fori_loop(chunks, 2 * chunks, first_layer, 0)

    def rest(step, _):
        for which in (0, 1, 2, 3, 4, 5):
            lane(which, step)
        return 0

    lax.fori_loop(3 + 2 * chunks, 3 + 2 * chunks + n, rest, 0)

    own = pl.ds(pl.multiple_of(me * rows, rows), rows)
    own_deep = pl.ds(pl.multiple_of(me * 2 * deep, 2 * deep), 2 * deep)
    outs = [
        pltpu.make_async_copy(gg.at[:, own, :], og, osem.at[0]),
        pltpu.make_async_copy(gu.at[:, own, :], ou, osem.at[1]),
        pltpu.make_async_copy(gd.at[:, own_deep, :], od, osem.at[2]),
    ]
    for copy in outs:
        copy.start()
    for copy in outs:
        copy.wait()


def gradients(n, x, dy, w):
    wg, wu, wd = w
    tokens, width = x.shape
    layers, _, hidden = wg.shape
    chunk, wide_cols = hidden // 8, hidden // 4
    rows, deep = width // n, hidden // n // 2
    anywhere = pl.BlockSpec(memory_space=pl.ANY)
    state = pltpu.VMEM((tokens, width), BF16)
    turned = pltpu.VMEM((width, tokens), BF16)
    hiddens = pltpu.VMEM((tokens, chunk), BF16)
    outs = pl.pallas_call(
        functools.partial(gradients_kernel, n),
        out_shape=[
            jax.ShapeDtypeStruct((layers, rows, hidden), BF16),
            jax.ShapeDtypeStruct((layers, rows, hidden), BF16),
            jax.ShapeDtypeStruct((layers, 2 * deep, width), BF16),
            jax.ShapeDtypeStruct((8, 128), F32),
            jax.ShapeDtypeStruct((2, hidden // chunk, tokens, chunk), BF16),
        ],
        in_specs=[anywhere] * 5,
        out_specs=[anywhere] * 3 + [pl.BlockSpec(memory_space=pltpu.VMEM), anywhere],
        scratch_shapes=[
            state, state, turned, state, turned,
            pltpu.VMEM((tokens, width), F32),
            pltpu.VMEM((2, width, chunk), BF16),
            pltpu.VMEM((2, width, chunk), BF16),
            pltpu.VMEM((2, chunk, width), BF16),
            hiddens, pltpu.VMEM((2, tokens, chunk), BF16), pltpu.VMEM((2, tokens, chunk), BF16),
            pltpu.VMEM(wg.shape, BF16),
            pltpu.VMEM(wu.shape, BF16),
            pltpu.VMEM(wd.shape, BF16),
            pltpu.VMEM((2, 4, n - 1, rows, wide_cols), BF16),
            pltpu.VMEM((2, 2, n - 1, deep, width // 2), BF16),
            pltpu.SemaphoreType.DMA((2, 3)),
            pltpu.SemaphoreType.DMA((2,)),
            pltpu.SemaphoreType.DMA((3,)),
            pltpu.SemaphoreType.DMA((2, 6)),
            pltpu.SemaphoreType.DMA((2, 6, n - 1)),
            pltpu.SemaphoreType.REGULAR((2, 6)),
            pltpu.SemaphoreType.DMA((2, 2)),
        ],
        compiler_params=pltpu.CompilerParams(collective_id=0, has_side_effects=True, vmem_limit_bytes=67_043_328),
        name="gradients",
    )(x, dy, *w)
    return outs[:3], outs[3]


def update_kernel(n, layers, count, *refs):
    ssq, g, w, m, v = refs[0], refs[1:4], refs[4:7], refs[7:10], refs[10:13]
    nw, nm, nv = refs[13:16], refs[16:19], refs[19:22]
    gs, ws, ms, vs = refs[22:25], refs[25:28], refs[28:31], refs[31:34]
    slots, load_sem, store_sem, own_sem, ssq_send, ssq_recv, send_sem, recv_sem = refs[34:]
    me = lax.axis_index("dp")
    right, left = lax.rem(me + 1, n), lax.rem(me + n - 1, n)
    blocks = [(i, l) for l in range(layers) for i in range(3)]
    rows = [r.shape[1] for r in g]

    loads = {}
    for k, (i, l) in enumerate(blocks):
        own = pl.ds(pl.multiple_of(me * rows[i], rows[i]), rows[i])
        pairs = ((g[i].at[l], gs[i].at[l]), (w[i].at[l, own], ws[i].at[l]), (m[i].at[l], ms[i].at[l]), (v[i].at[l], vs[i].at[l]))
        loads[k] = [pltpu.make_async_copy(src, dst, load_sem.at[k, j]) for j, (src, dst) in enumerate(pairs)]
        for copy in loads[k]:
            copy.start()

    barrier = pltpu.get_barrier_semaphore()
    for d in range(1, n):
        pl.semaphore_signal(barrier, inc=1, device_id={"dp": lax.rem(me + d, n)}, device_id_type=MESH)
    pl.semaphore_wait(barrier, n - 1)

    sums = [
        pltpu.make_async_remote_copy(
            src_ref=ssq, dst_ref=slots.at[d], send_sem=ssq_send.at[d], recv_sem=ssq_recv.at[d],
            device_id={"dp": lax.rem(me + d, n)}, device_id_type=MESH,
        )
        for d in range(1, n)
    ]
    for copy in sums:
        copy.start()
    total = ssq[...]
    for d, copy in enumerate(sums, 1):
        copy.wait()
        total = total + slots[d]
    total = jnp.sum(jnp.sum(total, axis=1, keepdims=True), axis=0, keepdims=True)
    factor = jnp.minimum(1.0, 0.5 * lax.rsqrt(total / count + 1e-30))

    def piece(ref, i, l, owner, way):
        half = rows[i] // 2
        return ref.at[l, pl.ds(pl.multiple_of(owner * rows[i] + way * half, half), half)]

    def hop(k, way, step, first):
        i, l = blocks[k]
        owner = lax.rem(me + (n - step if way == 0 else step), n)
        half = rows[i] // 2
        src = ws[i].at[l, pl.ds(way * half, half)] if first else piece(nw[i], i, l, owner, way)
        return pltpu.make_async_remote_copy(
            src_ref=src, dst_ref=piece(nw[i], i, l, owner, way), send_sem=send_sem.at[way, k, step], recv_sem=recv_sem.at[way, k, step],
            device_id={"dp": (right, left)[way]}, device_id_type=MESH,
        )

    stores = []
    for k, (i, l) in enumerate(blocks):
        for copy in loads[k]:
            copy.wait()
        tile = 32

        def body(t, _, i=i, l=l, tile=tile):
            at = (l, pl.ds(pl.multiple_of(t * tile, tile), tile))
            grad = gs[i][at].astype(F32) * factor
            wide = ws[i][at].astype(F32)
            new_m = 0.9 * ms[i][at] + 0.1 * grad
            new_v = 0.95 * vs[i][at] + 0.05 * grad * grad
            ms[i][at] = new_m
            vs[i][at] = new_v
            step = new_m * lax.rsqrt(new_v + 1e-8) + 0.1 * wide
            ws[i][at] = (wide - 0.02 * step).astype(BF16)
            return 0

        lax.fori_loop(0, rows[i] // tile, body, 0)
        for way in range(2):
            hop(k, way, 0, True).start()
        own = pl.ds(pl.multiple_of(me * rows[i], rows[i]), rows[i])
        pairs = ((ws[i].at[l], nw[i].at[l, own]), (ms[i].at[l], nm[i].at[l]), (vs[i].at[l], nv[i].at[l]))
        for j, (src, dst) in enumerate(pairs):
            stores.append(pltpu.make_async_copy(src, dst, store_sem.at[k, j]))
            stores[-1].start()

    for step in range(1, n):
        for k in range(len(blocks)):
            for way in range(2):
                hop(k, way, step - 1, False).wait_recv()
                if step < n - 1:
                    hop(k, way, step, False).start()
    for step in range(n - 1):
        for k in range(len(blocks)):
            for way in range(2):
                hop(k, way, step, step == 0).wait_send()
    for copy in stores:
        copy.wait()


def update(n, ssq, g, w, m, v):
    layers = w[0].shape[0]
    count = float(sum(t.size for t in w))
    blocks = 3 * layers
    anywhere = pl.BlockSpec(memory_space=pl.ANY)
    g, w, m, v = ([pltpu.with_memory_space_constraint(t, pltpu.HBM) for t in ts] for ts in (g, w, m, v))
    outs = pl.pallas_call(
        functools.partial(update_kernel, n, layers, count),
        out_shape=[jax.ShapeDtypeStruct(t.shape, t.dtype) for t in (*w, *m, *v)],
        in_specs=[pl.BlockSpec(memory_space=pltpu.VMEM)] + [pl.BlockSpec(memory_space=pltpu.HBM)] * 12,
        out_specs=[anywhere] * 9,
        scratch_shapes=[pltpu.VMEM(t.shape, t.dtype) for t in (*g, *g, *m, *v)]
        + [
            pltpu.VMEM((n, *ssq.shape), F32),
            pltpu.SemaphoreType.DMA((blocks, 4)),
            pltpu.SemaphoreType.DMA((blocks, 3)),
            pltpu.SemaphoreType.DMA((1,)),
            pltpu.SemaphoreType.DMA((n,)),
            pltpu.SemaphoreType.DMA((n,)),
            pltpu.SemaphoreType.DMA((2, blocks, n - 1)),
            pltpu.SemaphoreType.DMA((2, blocks, n - 1)),
        ],
        compiler_params=pltpu.CompilerParams(collective_id=1, has_side_effects=True, vmem_limit_bytes=16 * 2**20),
        name="update",
    )(ssq, *g, *w, *m, *v)
    return tuple(outs)


def settle_kernel(*refs):
    *arrays, sems = refs
    half = len(arrays) // 2
    copies = [pltpu.make_async_copy(arrays[k], arrays[half + k], sems.at[k]) for k in range(half)]
    for copy in copies:
        copy.start()
    for copy in copies:
        copy.wait()


def settle(results):
    anywhere = pl.BlockSpec(memory_space=pl.ANY)
    return pl.pallas_call(
        settle_kernel,
        out_shape=[jax.ShapeDtypeStruct(t.shape, t.dtype) for t in results],
        in_specs=[anywhere] * len(results),
        out_specs=[anywhere] * len(results),
        scratch_shapes=[pltpu.SemaphoreType.DMA((len(results),))],
        compiler_params=pltpu.CompilerParams(vmem_limit_bytes=2**20),
        name="settle",
    )(*results)


def solution(mesh):
    n = mesh.shape["dp"]

    def device(x, dy, *arrays):
        w, m, v = (arrays[i : i + 3] for i in (0, 3, 6))
        g, ssq = gradients(n, x[0], dy[0], w)
        return tuple(settle(update(n, ssq, g, w, m, v)))

    whole, part = P(None, None, None), P(None, "dp", None)
    return jax.shard_map(
        device,
        mesh=mesh,
        in_specs=(P(("rep", "dp")), P(("rep", "dp"))) + (whole,) * 3 + (part,) * 6,
        out_specs=(P("rep"),) * 3 + (P("rep", "dp"),) * 6,
        check_vma=False,
    )
```
